32 devices in a mesh: win: 4 (over x, core), obs: 8 (over z, y).
Axes of the slice: x: 2, y: 2, z: 4, core: 2. Of those that a mesh axis runs over, the one named last changes fastest.
Arguments:
- predictors: float32 [4, 8, 262144], P('win', None, 'obs'), may hold values from -8 to 8
- departures: float32 [4, 262144], P('win', 'obs'), may hold values from -30 to 30
- channel: int32 [4, 262144], P('win', 'obs'), may hold values from 0 to 299
- decay_rate: float32 [4, 300], P('win'), may hold values from 0.5 to 1
- ridge_counts: int32 [4, 300], P('win'), may hold values from 219 to 874
Outputs:
- coefficients: float32 [4, 8, 300], P('win')
- corrected: float32 [4, 262144], P('win', 'obs')
The draws below stay inside these ranges and needn't reach their ends.
All inputs are finite; a program needn't handle non-finite values.
Results may differ from the reference program's by a relative error of at most 0.00013.
Values sent between devices are 32-bit elements; how exact they have to be, the bound alone decides.
A program may use at most 64 MiB of HBM per device.

```python
import math
import jax
import jax.numpy as jnp
from jax import lax

C = 300
K = 8
ROUNDS = 3
WINDOWS = 4
OBS = 262144


def pick_rows(coef_table, labels):
    return jnp.take(coef_table, labels, axis=0)


def observe_world(key):
    base = jax.random.fold_in(key, 4242)
    subkeys = jax.random.split(base, 5)
    channel = jax.random.randint(subkeys[0], (WINDOWS, OBS), 0, C, dtype=jnp.int32)
    predictors = jax.random.normal(subkeys[2], (WINDOWS, K, OBS))
    noise_term = jax.random.normal(subkeys[4], (WINDOWS, OBS))
    predictors = jnp.clip(predictors, -8.0, 8.0)
    truth_table = 0.5 * jax.random.normal(subkeys[3], (WINDOWS, C, K))
    picked = jax.vmap(pick_rows)(truth_table, channel)
    signal = jnp.sum(picked * jnp.transpose(predictors, (0, 2, 1)), axis=2)
    departures = jnp.clip(signal + noise_term, -30.0, 30.0)
    return (channel, predictors.astype(jnp.float32), departures.astype(jnp.float32))


def draw_channel(key, part):
    return observe_world(key)[0]


def draw_predictors(key, part):
    return observe_world(key)[1]


def draw_departures(key, part):
    return observe_world(key)[2]


def touch_ends(values, own_key, low, top_value):
    longest = values.shape.index(max(values.shape))
    spots = []
    for shift in (0, 1):
        where = [jax.random.randint(jax.random.fold_in(own_key, axis), (), 0, length) for axis, length in enumerate(values.shape)]
        where[longest] = (where[longest] + shift) % values.shape[longest]
        spots.append(tuple(where))
    return values.at[spots[0]].set(low).at[spots[1]].set(top_value)


def levels(stream_key, extent, cuts, smallest, high):
    def one(axis_at, parts):
        steps = jax.random.uniform(jax.random.fold_in(jax.random.fold_in(stream_key, 6), axis_at), (parts,), jnp.float32, smallest / len(cuts), high / len(cuts))
        return jnp.repeat(jnp.exp(steps), extent[axis_at] // parts).reshape((-1,) + (1,) * (len(extent) - axis_at - 1))

    gain = one(*cuts[0])
    for cut in cuts[1:]:
        gain = gain * one(*cut)
    return gain


def setup_inputs(seed: int = 0) -> dict:
    arg_keys = jax.random.split(jax.random.key(seed), 6)
    predictors = draw_predictors(jax.random.fold_in(arg_keys[5], 71), 0)
    departures = draw_departures(jax.random.fold_in(arg_keys[5], 71), 0)
    channel = draw_channel(jax.random.fold_in(arg_keys[5], 71), 0)
    decay_rate = jnp.clip(jnp.exp(math.log(1.0) - 0.6931472 * jax.random.uniform(arg_keys[3], (WINDOWS, C), jnp.float32) ** levels(arg_keys[3], (WINDOWS, C), ((0, 4),), -0.2, 0.2)), 0.5, 1.0)
    ridge_counts = touch_ends(jax.random.randint(arg_keys[4], (WINDOWS, C), OBS // (4 * C) + 1, OBS // C + 2), jax.random.fold_in(arg_keys[4], 1), OBS // (4 * C) + 1, (OBS // C + 2) - 1).astype(jnp.int32)
    return {"predictors": predictors, "departures": departures, "channel": channel, "decay_rate": decay_rate, "ridge_counts": ridge_counts}


huber_edge = 1.5

def fit_rows(predictors, coeffs, channel):
    return lax.optimization_barrier(jnp.sum(predictors * jnp.take(coeffs, channel, axis=1), axis=0))

def build_features(predictors, departure, weights):
    weighted = predictors * weights[None, :]
    gram_rows = (weighted[:, None, :] * predictors[None, :, :]).reshape(-1, predictors.shape[1])
    moment_rows = weighted * departure[None, :]
    return jnp.concatenate([gram_rows, moment_rows], axis=0)

def solve_small(matrix, right_side):
    dimension = right_side.shape[0]
    factor = {}
    for column in range(dimension):
        pivot_square = matrix[column, column] - sum((factor[column, middle] * factor[column, middle] for middle in range(column)))
        pivot_root = jnp.sqrt(pivot_square)
        factor[column, column] = pivot_root
        for row_index in range(column + 1, dimension):
            partial_sum = matrix[row_index, column] - sum((factor[row_index, middle] * factor[column, middle] for middle in range(column)))
            factor[row_index, column] = partial_sum / pivot_root
    forward = []
    for row_index in range(dimension):
        entry_value = right_side[row_index] - sum((factor[row_index, middle] * forward[middle] for middle in range(row_index)))
        forward.append(entry_value / factor[row_index, row_index])
    solution = [None] * dimension
    for row_index in reversed(range(dimension)):
        entry_value = forward[row_index] - sum((factor[middle, row_index] * solution[middle] for middle in range(row_index + 1, dimension)))
        solution[row_index] = entry_value / factor[row_index, row_index]
    return jnp.stack(solution, axis=0)

def solve_channels(summed, ridges):
    dimension = K
    matrix = summed[:dimension * dimension].reshape(dimension, dimension, -1)
    matrix = matrix + ridges[None, None, :] * jnp.eye(dimension, dtype=jnp.float32)[:, :, None]
    return solve_small(matrix, summed[dimension * dimension:])

def reference(predictors, departures, channel, decay_rate, ridge_counts):
    coeffs = jnp.zeros((WINDOWS, K, C), jnp.float32)
    for round_index in range(ROUNDS):
        carried = jnp.zeros((K * K + K, C), jnp.float32)
        updated = []
        for window in range(WINDOWS):
            residual = departures[window] - fit_rows(predictors[window], coeffs[window], channel[window])
            weights = huber_edge / jnp.maximum(jnp.abs(residual), huber_edge)
            features = build_features(predictors[window], departures[window], weights)
            summed = jax.ops.segment_sum(features.T, channel[window], num_segments=C).T
            carried = decay_rate[window][None, :] * carried + summed
            updated.append(solve_channels(carried, ridge_counts[window].astype(jnp.float32)))
        coeffs = jnp.stack(updated, axis=0)
    fitted = jnp.stack([fit_rows(predictors[window], coeffs[window], channel[window]) for window in range(WINDOWS)], axis=0)
    return (coeffs, departures - fitted)
```

```python
import functools

import jax
import jax.numpy as jnp
from jax import lax
from jax.experimental import pallas as pl
from jax.experimental.pallas import tpu as pltpu
from jax.sharding import PartitionSpec as P

ROUNDS = 3
LANES = 128
GROUPS = 16

huber_edge = 1.5

MESH = pl.DeviceIdType.MESH


def ceil_to(value, unit):
    return (value + unit - 1) // unit * unit


def gather_lanes(table, index):
    return jnp.take_along_axis(table, index, axis=1, mode="promise_in_bounds")


def fit_group(columns, labels, tables):
    low = jnp.bitwise_and(labels, LANES - 1)
    high = jnp.right_shift(labels, 7)
    picked = gather_lanes(tables[0], low)
    for slab in range(1, len(tables)):
        picked = jnp.where(high == slab, gather_lanes(tables[slab], low), picked)
    return jnp.sum(columns * picked, axis=0, keepdims=True)


def entry_place(a, b, dim):
    shift = (a - b) % dim
    if shift <= dim // 2:
        return shift * dim + a
    return (dim - shift) * dim + b


def kernel(
    sizes,
    rows_ref,
    depart_ref,
    label_ref,
    decay_ref,
    ridge_ref,
    coef_ref,
    corrected_ref,
    acc,
    stats,
    beta,
    ridge_row,
    decays,
    parts,
    totals,
    chained,
    decay_send,
    decay_recv,
    part_send,
    part_recv,
    total_send,
    total_recv,
    chain_send,
    chain_recv,
):
    dim, channels, n_win, n_obs, slabs = sizes
    width = slabs * LANES
    hot_rows = ceil_to(channels, 16)
    owners = stats.shape[0] // dim
    steps = depart_ref.shape[0] // GROUPS
    chunk = GROUPS * LANES
    w = lax.axis_index("win")
    o = lax.axis_index("obs")

    barrier = pltpu.get_barrier_semaphore()
    for step in range(1, n_obs):
        pl.semaphore_signal(
            barrier, inc=1, device_id={"obs": lax.rem(o + step, n_obs)}, device_id_type=MESH
        )
    for step in range(1, n_win):
        pl.semaphore_signal(
            barrier, inc=1, device_id={"win": lax.rem(w + step, n_win)}, device_id_type=MESH
        )
    pl.semaphore_wait(barrier, n_obs + n_win - 2)

    def decay_copy(step, slot, target):
        return pltpu.make_async_remote_copy(
            src_ref=decays.at[slot],
            dst_ref=decays.at[slot],
            send_sem=decay_send.at[step],
            recv_sem=decay_recv.at[step],
            device_id={"win": target},
            device_id_type=MESH,
        )

    decays[w] = jnp.zeros((dim, width), jnp.float32)
    decays[w, :, 0:channels] = jnp.broadcast_to(decay_ref[...], (dim, channels))
    for step in range(1, n_win):
        decay_copy(step, w, lax.rem(w + step, n_win)).start()

    ridge_row[...] = jnp.ones_like(ridge_row)
    ridge_row[:, 0:channels] = ridge_ref[...].astype(jnp.float32)
    beta[...] = jnp.zeros_like(beta)

    def tables_now():
        return [beta[:, slab * LANES : (slab + 1) * LANES] for slab in range(slabs)]

    def wide_row(ref, row):
        return jnp.broadcast_to(ref[pl.ds(row, 1), :], (dim, LANES))

    def accumulate(step, tables):
        fits, departs, labels = [], [], []
        columns_all = []
        for group in range(GROUPS):
            row = step * GROUPS + group
            begin = pl.multiple_of(row * LANES, LANES)
            columns = rows_ref[:, pl.ds(begin, LANES)]
            label = wide_row(label_ref, row)
            depart = wide_row(depart_ref, row)
            residual = depart - fit_group(columns, label, tables)
            weight = huber_edge / jnp.maximum(jnp.abs(residual), huber_edge)
            columns_all.append(columns)
            fits.append(columns * weight)
            departs.append(depart)
            labels.append(label)
        columns = jnp.concatenate(columns_all, axis=1)
        weighted = jnp.concatenate(fits, axis=1)
        depart = jnp.concatenate(departs, axis=1)
        label = jnp.concatenate(labels, axis=1)
        features = [weighted * columns]
        for shift in range(1, dim // 2 + 1):
            features.append(weighted * pltpu.roll(columns, shift, axis=0))
        features.append(weighted * depart)
        features = jnp.concatenate(features, axis=0)
        high = features.astype(jnp.bfloat16)
        low = (features - high.astype(jnp.float32)).astype(jnp.bfloat16)
        pair = jnp.concatenate([high, low], axis=0)
        hots = []
        one, nought = jnp.bfloat16(1), jnp.bfloat16(0)
        for base in range(0, hot_rows, 256):
            here = min(256, hot_rows - base)
            shifted = (label - base).astype(jnp.float32).astype(jnp.bfloat16)
            ids = lax.broadcasted_iota(jnp.int32, (here, LANES), 0)
            ids = ids.astype(jnp.float32).astype(jnp.bfloat16)
            shifted16 = jnp.concatenate([shifted, shifted], axis=0)
            for part in range(0, here, 2 * dim):
                id_tile = jnp.concatenate([ids[part : part + 2 * dim]] * GROUPS, axis=1)
                hots.append(jnp.where(id_tile == shifted16, one, nought))
        hot = jnp.concatenate(hots, axis=0)
        acc[:, 0:hot_rows] += lax.dot_general(
            pair, hot, (((1,), (1,)), ((), ())), preferred_element_type=jnp.float32
        )

    def part_copy(r, group, slot):
        return pltpu.make_async_remote_copy(
            src_ref=stats.at[pl.ds(group * dim, dim)],
            dst_ref=parts.at[r, slot],
            send_sem=part_send.at[r, group],
            recv_sem=part_recv.at[r, slot],
            device_id={"obs": group},
            device_id_type=MESH,
        )

    def total_copy(r, step, slot, target):
        return pltpu.make_async_remote_copy(
            src_ref=totals.at[r, slot],
            dst_ref=totals.at[r, slot],
            send_sem=total_send.at[r, step],
            recv_sem=total_recv.at[r, step],
            device_id={"win": target},
            device_id_type=MESH,
        )

    def chain_copy(r, step, slot, target):
        return pltpu.make_async_remote_copy(
            src_ref=chained.at[r, slot],
            dst_ref=chained.at[r, slot],
            send_sem=chain_send.at[r, step],
            recv_sem=chain_recv.at[r, slot],
            device_id={"obs": target},
            device_id_type=MESH,
        )

    def combine(r):
        half = stats.shape[0]
        stats[...] = acc[0:half] + acc[half:]
        for group in range(owners):

            @pl.when(o != group)
            def _():
                part_copy(r, group, o).start()

        @pl.when(o < owners)
        def _():
            parts[r, o] = stats[pl.ds(pl.multiple_of(o * dim, dim), dim), :]
            for step in range(1, n_obs):
                part_copy(r, 0, lax.rem(o + step, n_obs)).wait_recv()
            total = parts[r, 0]
            for source in range(1, n_obs):
                total = total + parts[r, source]
            totals[r, w] = total
            for step in range(1, n_win):
                total_copy(r, step, w, lax.rem(w + step, n_win)).start()
            for step in range(1, n_win):
                total_copy(r, step, lax.rem(w + n_win - step, n_win), w).wait_recv()
            carried = totals[r, 0]
            for window in range(1, n_win):
                further = decays[window] * carried + totals[r, window]
                carried = jnp.where(window <= w, further, carried)
            chained[r, o] = carried
            for step in range(1, n_obs):
                chain_copy(r, step, o, lax.rem(o + step, n_obs)).start()

        for group in range(owners):

            @pl.when(o != group)
            def _():
                chain_copy(r, 1, group, o).wait_recv()

        for group in range(owners):

            @pl.when(o != group)
            def _():
                part_copy(r, group, o).wait_send()

        @pl.when(o < owners)
        def _():
            for step in range(1, n_win):
                total_copy(r, step, w, w).wait_send()
            for step in range(1, n_obs):
                chain_copy(r, step, o, o).wait_send()

    def solve(r):
        def entry(place):
            return chained[r, place // dim, pl.ds(place % dim, 1), :]

        unit = {}
        scaled = {}
        inverse = []
        for column in range(dim):
            pivot = entry(entry_place(column, column, dim)) + ridge_row[...]
            for middle in range(column):
                pivot = pivot - unit[column, middle] * scaled[column, middle]
            inverse.append(1.0 / pivot)
            for row in range(column + 1, dim):
                value = entry(entry_place(row, column, dim))
                for middle in range(column):
                    value = value - unit[column, middle] * scaled[row, middle]
                scaled[row, column] = value
                unit[row, column] = value * inverse[column]
        forward = []
        moment = (dim // 2 + 1) * dim
        for row in range(dim):
            value = entry(moment + row)
            for middle in range(row):
                value = value - unit[row, middle] * forward[middle]
            forward.append(value)
        answer = [None] * dim
        for row in reversed(range(dim)):
            value = forward[row] * inverse[row]
            for middle in range(row + 1, dim):
                value = value - unit[middle, row] * answer[middle]
            answer[row] = value
            beta[row : row + 1, :] = value

    for step in range(1, n_win):
        decay_copy(step, lax.rem(w + n_win - step, n_win), w).wait_recv()
    for step in range(1, n_win):
        decay_copy(step, w, w).wait_send()

    def one_round(r, carry):
        acc[...] = jnp.zeros_like(acc)
        tables = tables_now()

        def one_step(step, inner):
            accumulate(step, tables)
            return inner

        lax.fori_loop(0, steps, one_step, 0)
        combine(r)
        solve(r)
        return carry

    lax.fori_loop(0, ROUNDS, one_round, 0)

    coef_ref[...] = beta[:, 0:channels]
    tables = tables_now()

    def correct(step, carry):
        for group in range(GROUPS):
            row = step * GROUPS + group
            begin = pl.multiple_of(row * LANES, LANES)
            columns = rows_ref[:, pl.ds(begin, LANES)]
            fitted = fit_group(columns, wide_row(label_ref, row), tables)
            corrected_ref[pl.ds(row, 1), :] = depart_ref[pl.ds(row, 1), :] - fitted
        return carry

    lax.fori_loop(0, steps, correct, 0)


def body(n_win, n_obs, predictors, departures, channel, decay_rate, ridge_counts):
    channels = decay_rate.shape[1]
    dim = predictors.shape[1]
    total_rows = predictors.shape[2]
    slabs = ceil_to(channels, LANES) // LANES
    width = slabs * LANES
    owners = dim // 2 + 2
    packed = owners * dim
    assert n_obs >= owners and total_rows % (GROUPS * LANES) == 0
    vmem = pl.BlockSpec(memory_space=pltpu.VMEM)
    dma = pltpu.SemaphoreType.DMA
    coeffs, corrected = pl.pallas_call(
        functools.partial(kernel, (dim, channels, n_win, n_obs, slabs)),
        out_shape=(
            jax.ShapeDtypeStruct((dim, channels), jnp.float32),
            jax.ShapeDtypeStruct((total_rows // LANES, LANES), jnp.float32),
        ),
        in_specs=[vmem] * 5,
        out_specs=(vmem, vmem),
        scratch_shapes=[
            pltpu.VMEM((2 * packed, width), jnp.float32),
            pltpu.VMEM((packed, width), jnp.float32),
            pltpu.VMEM((dim, width), jnp.float32),
            pltpu.VMEM((1, width), jnp.float32),
            pltpu.VMEM((n_win, dim, width), jnp.float32),
            pltpu.VMEM((ROUNDS, n_obs, dim, width), jnp.float32),
            pltpu.VMEM((ROUNDS, n_win, dim, width), jnp.float32),
            pltpu.VMEM((ROUNDS, owners, dim, width), jnp.float32),
            dma((n_win,)),
            dma((n_win,)),
            dma((ROUNDS, owners)),
            dma((ROUNDS, n_obs)),
            dma((ROUNDS, n_win)),
            dma((ROUNDS, n_win)),
            dma((ROUNDS, n_obs)),
            dma((ROUNDS, owners)),
        ],
        compiler_params=pltpu.CompilerParams(
            collective_id=0, has_side_effects=True, vmem_limit_bytes=48 * 1024 * 1024
        ),
    )(
        predictors.reshape(dim, total_rows),
        departures.reshape(total_rows // LANES, LANES),
        channel.reshape(total_rows // LANES, LANES),
        decay_rate,
        ridge_counts,
    )
    return (coeffs[None], corrected.reshape(1, total_rows))


def solution(mesh):
    placed = (
        P("win", None, "obs"),
        P("win", "obs"),
        P("win", "obs"),
        P("win", None),
        P("win", None),
    )
    return jax.shard_map(
        functools.partial(body, mesh.shape["win"], mesh.shape["obs"]),
        mesh=mesh,
        in_specs=placed,
        out_specs=(P("win", None, None), P("win", "obs")),
        check_vma=False,
    )
```

```python
import functools

import jax
import jax.numpy as jnp
from jax import lax
from jax.experimental import pallas as pl
from jax.experimental.pallas import tpu as pltpu
from jax.sharding import PartitionSpec as P

ROUNDS = 3
LANES = 128
GROUPS = 16

huber_edge = 1.5

MESH = pl.DeviceIdType.MESH


def ceil_to(value, unit):
    return (value + unit - 1) // unit * unit


def gather_lanes(table, index):
    return jnp.take_along_axis(table, index, axis=1, mode="promise_in_bounds")


def fit_group(columns, labels, tables):
    low = jnp.bitwise_and(labels, LANES - 1)
    high = jnp.right_shift(labels, 7)
    picked = gather_lanes(tables[0], low)
    for slab in range(1, len(tables)):
        picked = jnp.where(high == slab, gather_lanes(tables[slab], low), picked)
    return jnp.sum(columns * picked, axis=0, keepdims=True)


def entry_place(a, b, dim):
    shift = (a - b) % dim
    if shift <= dim // 2:
        return shift * dim + a
    return (dim - shift) * dim + b


def kernel(
    sizes,
    rows_hbm,
    depart_hbm,
    label_hbm,
    decay_ref,
    ridge_ref,
    coef_ref,
    corrected_ref,
    rows_ref,
    depart_ref,
    label_ref,
    acc,
    stats,
    betas,
    ridge_all,
    ridge_slab,
    decays,
    parts,
    totals,
    chained,
    load_sem,
    decay_send,
    decay_recv,
    part_send,
    part_recv,
    total_send,
    total_recv,
    beta_send,
    beta_recv,
):
    dim, channels, n_win, n_obs, slabs, half = sizes
    width = slabs * LANES
    packed = stats.shape[1]
    first = (n_obs - slabs) // 2
    steps = depart_ref.shape[0] // GROUPS
    chunk = GROUPS * LANES
    w = lax.axis_index("win")
    o = lax.axis_index("obs")

    barrier = pltpu.get_barrier_semaphore()
    for step in range(1, n_obs):
        pl.semaphore_signal(
            barrier, inc=1, device_id={"obs": lax.rem(o + step, n_obs)}, device_id_type=MESH
        )
    for step in range(1, n_win):
        pl.semaphore_signal(
            barrier, inc=1, device_id={"win": lax.rem(w + step, n_win)}, device_id_type=MESH
        )

    def loads(step):
        begin = pl.multiple_of(step * chunk, chunk)
        some = pl.ds(pl.multiple_of(step * GROUPS, GROUPS), GROUPS)
        return [
            pltpu.make_async_copy(
                rows_hbm.at[:, pl.ds(begin, chunk)],
                rows_ref.at[:, pl.ds(begin, chunk)],
                load_sem.at[0, step],
            ),
            pltpu.make_async_copy(depart_hbm.at[some], depart_ref.at[some], load_sem.at[1, step]),
            pltpu.make_async_copy(label_hbm.at[some], label_ref.at[some], load_sem.at[2, step]),
        ]

    def start_loads(step, carry):
        for load in loads(step):
            load.start()
        return carry

    lax.fori_loop(0, steps, start_loads, 0)

    def decay_copy(step, slot, target):
        return pltpu.make_async_remote_copy(
            src_ref=decays.at[slot],
            dst_ref=decays.at[slot],
            send_sem=decay_send.at[step],
            recv_sem=decay_recv.at[step],
            device_id={"win": target},
            device_id_type=MESH,
        )

    decays[w] = jnp.zeros((dim, width), jnp.float32)
    decays[w, :, 0:channels] = jnp.broadcast_to(decay_ref[...], (dim, channels))
    ridge_all[...] = jnp.ones_like(ridge_all)
    ridge_all[:, 0:channels] = ridge_ref[...].astype(jnp.float32)
    for slab in range(slabs):
        ridge_slab[slab] = ridge_all[:, slab * LANES : (slab + 1) * LANES]

    def tables_now(r):
        return [betas[r, slab] for slab in range(slabs)]

    def wide_row(ref, row):
        return jnp.broadcast_to(ref[pl.ds(row, 1), :], (dim, LANES))

    def accumulate(step, tables):
        fits, departs, labels = [], [], []
        columns_all = []
        for group in range(GROUPS):
            row = step * GROUPS + group
            begin = pl.multiple_of(row * LANES, LANES)
            columns = rows_ref[:, pl.ds(begin, LANES)]
            label = wide_row(label_ref, row)
            depart = wide_row(depart_ref, row)
            residual = depart
            if tables is not None:
                residual = depart - fit_group(columns, label, tables)
            weight = huber_edge / jnp.maximum(jnp.abs(residual), huber_edge)
            columns_all.append(columns)
            fits.append(columns * weight)
            departs.append(depart)
            labels.append(label)
        columns = jnp.concatenate(columns_all, axis=1)
        weighted = jnp.concatenate(fits, axis=1)
        depart = jnp.concatenate(departs, axis=1)
        label = jnp.concatenate(labels, axis=1)
        features = [weighted * columns]
        for shift in range(1, dim // 2 + 1):
            features.append(weighted * pltpu.roll(columns, shift, axis=0))
        features.append(weighted * depart)
        features = jnp.concatenate(features, axis=0)
        high = features.astype(jnp.bfloat16)
        low = (features - high.astype(jnp.float32)).astype(jnp.bfloat16)
        pair = jnp.concatenate([high, low], axis=0)
        upper = label >= half
        place = jnp.where(upper, label - half, label)
        place = place.astype(jnp.float32).astype(jnp.bfloat16)
        side = upper.astype(jnp.float32).astype(jnp.bfloat16)
        place = jnp.concatenate([place, place], axis=0)
        side = jnp.concatenate([side, side], axis=0)
        one, nought = jnp.bfloat16(1), jnp.bfloat16(0)
        is_upper = side > jnp.bfloat16(0.5)
        sides = [[], []]
        for part in range(0, 2 * packed, 2 * dim):
            tile = pair[part : part + 2 * dim]
            sides[0].append(jnp.where(is_upper, nought, tile))
            sides[1].append(jnp.where(is_upper, tile, nought))
        spread = jnp.concatenate(sides[0] + sides[1], axis=0)
        ids = lax.broadcasted_iota(jnp.int32, (half, LANES), 0)
        ids = ids.astype(jnp.float32).astype(jnp.bfloat16)
        hots = []
        for part in range(0, half, 2 * dim):
            id_tile = jnp.concatenate([ids[part : part + 2 * dim]] * GROUPS, axis=1)
            hots.append(jnp.where(id_tile == place, one, nought))
        hot = jnp.concatenate(hots, axis=0)
        acc[:, 0:half] += lax.dot_general(
            spread, hot, (((1,), (1,)), ((), ())), preferred_element_type=jnp.float32
        )

    def part_copy(r, slab, slot):
        return pltpu.make_async_remote_copy(
            src_ref=stats.at[slab],
            dst_ref=parts.at[r, slot],
            send_sem=part_send.at[r, slab],
            recv_sem=part_recv.at[r, slot],
            device_id={"obs": first + slab},
            device_id_type=MESH,
        )

    def total_copy(r, step, slot, target):
        return pltpu.make_async_remote_copy(
            src_ref=totals.at[r, slot],
            dst_ref=totals.at[r, slot],
            send_sem=total_send.at[r, step],
            recv_sem=total_recv.at[r, step],
            device_id={"win": target},
            device_id_type=MESH,
        )

    def beta_copy(r, step, slab, target):
        return pltpu.make_async_remote_copy(
            src_ref=betas.at[r, slab],
            dst_ref=betas.at[r, slab],
            send_sem=beta_send.at[r, step],
            recv_sem=beta_recv.at[r, slab],
            device_id={"obs": target},
            device_id_type=MESH,
        )

    def combine(r):
        zeros = jnp.zeros((packed, width - acc.shape[1]), jnp.float32)
        sides = []
        for side in range(2):
            begin = side * 2 * packed
            both = acc[begin : begin + packed] + acc[begin + packed : begin + 2 * packed]
            sides.append(jnp.concatenate([both, zeros], axis=1))
        whole = sides[0] + pltpu.roll(sides[1], half, axis=1)
        for slab in range(slabs):
            stats[slab] = whole[:, slab * LANES : (slab + 1) * LANES]
        for slab in range(slabs):

            @pl.when(o != first + slab)
            def _():
                part_copy(r, slab, o).start()

        for slab in range(slabs):

            @pl.when(o == first + slab)
            def _():
                parts[r, o] = stats[slab]
                for step in range(1, n_obs):
                    part_copy(r, 0, lax.rem(o + step, n_obs)).wait_recv()
                total = parts[r, 0]
                for source in range(1, n_obs):
                    total = total + parts[r, source]
                totals[r, w] = total
                for step in range(1, n_win):
                    total_copy(r, step, w, lax.rem(w + step, n_win)).start()
                for step in range(1, n_win):
                    total_copy(r, step, lax.rem(w + n_win - step, n_win), w).wait_recv()
                lanes = slice(slab * LANES, (slab + 1) * LANES)
                carried = totals[r, 0]
                for window in range(1, n_win):
                    decay = jnp.concatenate([decays[window, :, lanes]] * (packed // dim), axis=0)
                    further = decay * carried + totals[r, window]
                    carried = jnp.where(window <= w, further, carried)
                chained[...] = carried
                solve(r, slab)
                for step in range(1, n_obs):
                    beta_copy(r, step, slab, lax.rem(o + step, n_obs)).start()

        for slab in range(slabs):

            @pl.when(o != first + slab)
            def _():
                beta_copy(r, 1, slab, o).wait_recv()

        for slab in range(slabs):

            @pl.when(o != first + slab)
            def _():
                part_copy(r, slab, o).wait_send()

            @pl.when(o == first + slab)
            def _():
                for step in range(1, n_win):
                    total_copy(r, step, w, w).wait_send()
                for step in range(1, n_obs):
                    beta_copy(r, step, slab, o).wait_send()

    def solve(r, slab):
        def entry(place):
            return chained[place : place + 1, :]

        unit = {}
        scaled = {}
        inverse = []
        for column in range(dim):
            pivot = entry(entry_place(column, column, dim)) + ridge_slab[slab]
            for middle in range(column):
                pivot = pivot - unit[column, middle] * scaled[column, middle]
            inverse.append(1.0 / pivot)
            for row in range(column + 1, dim):
                value = entry(entry_place(row, column, dim))
                for middle in range(column):
                    value = value - unit[column, middle] * scaled[row, middle]
                scaled[row, column] = value
                unit[row, column] = value * inverse[column]
        forward = []
        moment = (dim // 2 + 1) * dim
        for row in range(dim):
            value = entry(moment + row)
            for middle in range(row):
                value = value - unit[row, middle] * forward[middle]
            forward.append(value)
        answer = [None] * dim
        for row in reversed(range(dim)):
            value = forward[row] * inverse[row]
            for middle in range(row + 1, dim):
                value = value - unit[middle, row] * answer[middle]
            answer[row] = value
            betas[r, slab, row : row + 1, :] = value

    acc[...] = jnp.zeros_like(acc)

    def opening_step(step, carry):
        for load in loads(step):
            load.wait()
        accumulate(step, None)
        return carry

    lax.fori_loop(0, steps, opening_step, 0)

    pl.semaphore_wait(barrier, n_obs + n_win - 2)
    for step in range(1, n_win):
        decay_copy(step, w, lax.rem(w + step, n_win)).start()
    for step in range(1, n_win):
        decay_copy(step, lax.rem(w + n_win - step, n_win), w).wait_recv()
    for step in range(1, n_win):
        decay_copy(step, w, w).wait_send()
    combine(0)

    def one_round(r, carry):
        acc[...] = jnp.zeros_like(acc)
        tables = tables_now(r - 1)

        def one_step(step, inner):
            accumulate(step, tables)
            return inner

        lax.fori_loop(0, steps, one_step, 0)
        combine(r)
        return carry

    lax.fori_loop(1, ROUNDS, one_round, 0)

    tables = tables_now(ROUNDS - 1)
    coef_ref[...] = jnp.concatenate(tables, axis=1)[:, 0:channels]

    def correct(step, carry):
        for group in range(GROUPS):
            row = step * GROUPS + group
            begin = pl.multiple_of(row * LANES, LANES)
            columns = rows_ref[:, pl.ds(begin, LANES)]
            fitted = fit_group(columns, wide_row(label_ref, row), tables)
            corrected_ref[pl.ds(row, 1), :] = depart_ref[pl.ds(row, 1), :] - fitted
        return carry

    lax.fori_loop(0, steps, correct, 0)


def body(n_win, n_obs, predictors, departures, channel, decay_rate, ridge_counts):
    channels = decay_rate.shape[1]
    dim = predictors.shape[1]
    total_rows = predictors.shape[2]
    slabs = ceil_to(channels, LANES) // LANES
    width = slabs * LANES
    packed = (dim // 2 + 2) * dim
    half = ceil_to((channels + 1) // 2, 16)
    acc_width = ceil_to(half, LANES)
    steps = total_rows // (GROUPS * LANES)
    assert n_obs >= slabs and total_rows % (GROUPS * LANES) == 0
    assert half <= 256 and acc_width < width and 2 * half <= width
    vmem = pl.BlockSpec(memory_space=pltpu.VMEM)
    hbm = pl.BlockSpec(memory_space=pltpu.HBM)
    dma = pltpu.SemaphoreType.DMA
    lines = total_rows // LANES
    coeffs, corrected = pl.pallas_call(
        functools.partial(kernel, (dim, channels, n_win, n_obs, slabs, half)),
        out_shape=(
            jax.ShapeDtypeStruct((dim, channels), jnp.float32),
            jax.ShapeDtypeStruct((lines, LANES), jnp.float32),
        ),
        in_specs=[hbm] * 3 + [vmem] * 2,
        out_specs=(vmem, vmem),
        scratch_shapes=[
            pltpu.VMEM((dim, total_rows), jnp.float32),
            pltpu.VMEM((lines, LANES), jnp.float32),
            pltpu.VMEM((lines, LANES), jnp.int32),
            pltpu.VMEM((4 * packed, acc_width), jnp.float32),
            pltpu.VMEM((slabs, packed, LANES), jnp.float32),
            pltpu.VMEM((ROUNDS, slabs, dim, LANES), jnp.float32),
            pltpu.VMEM((1, width), jnp.float32),
            pltpu.VMEM((slabs, 1, LANES), jnp.float32),
            pltpu.VMEM((n_win, dim, width), jnp.float32),
            pltpu.VMEM((ROUNDS, n_obs, packed, LANES), jnp.float32),
            pltpu.VMEM((ROUNDS, n_win, packed, LANES), jnp.float32),
            pltpu.VMEM((packed, LANES), jnp.float32),
            dma((3, steps)),
            dma((n_win,)),
            dma((n_win,)),
            dma((ROUNDS, slabs)),
            dma((ROUNDS, n_obs)),
            dma((ROUNDS, n_win)),
            dma((ROUNDS, n_win)),
            dma((ROUNDS, n_obs)),
            dma((ROUNDS, slabs)),
        ],
        compiler_params=pltpu.CompilerParams(
            collective_id=0, has_side_effects=True, vmem_limit_bytes=48 * 1024 * 1024
        ),
    )(
        predictors.reshape(dim, total_rows),
        departures.reshape(lines, LANES),
        channel.reshape(lines, LANES),
        decay_rate,
        ridge_counts,
    )
    return (coeffs[None], corrected.reshape(1, total_rows))


def solution(mesh):
    placed = (
        P("win", None, "obs"),
        P("win", "obs"),
        P("win", "obs"),
        P("win", None),
        P("win", None),
    )
    return jax.shard_map(
        functools.partial(body, mesh.shape["win"], mesh.shape["obs"]),
        mesh=mesh,
        in_specs=placed,
        out_specs=(P("win", None, None), P("win", "obs")),
        check_vma=False,
    )
```

```python
import functools

import jax
import jax.numpy as jnp
from jax import lax
from jax.experimental import pallas as pl
from jax.experimental.pallas import tpu as pltpu
from jax.sharding import PartitionSpec as P

ROUNDS = 3
LANES = 128
GROUPS = 16

huber_edge = 1.5

MESH = pl.DeviceIdType.MESH


def ceil_to(value, unit):
    return (value + unit - 1) // unit * unit


def gather_lanes(table, index):
    return jnp.take_along_axis(table, index, axis=1, mode="promise_in_bounds")


def fit_group(columns, labels, tables):
    low = jnp.bitwise_and(labels, LANES - 1)
    high = jnp.right_shift(labels, 7)
    picked = gather_lanes(tables[0], low)
    for slab in range(1, len(tables)):
        picked = jnp.where(high == slab, gather_lanes(tables[slab], low), picked)
    return jnp.sum(columns * picked, axis=0, keepdims=True)


def entry_place(a, b, dim):
    shift = (a - b) % dim
    if shift <= dim // 2:
        return shift * dim + a
    return (dim - shift) * dim + b


def kernel(
    sizes,
    rows_hbm,
    depart_hbm,
    label_hbm,
    decay_ref,
    ridge_ref,
    coef_ref,
    corrected_ref,
    rows_ref,
    depart_ref,
    label_ref,
    acc,
    stats,
    betas,
    ridge_all,
    ridge_slab,
    decays,
    parts,
    totals,
    chained,
    load_sem,
    decay_send,
    decay_recv,
    part_send,
    part_recv,
    total_send,
    total_recv,
    beta_send,
    beta_recv,
):
    dim, channels, n_win, n_obs, slabs, half = sizes
    width = slabs * LANES
    packed = stats.shape[1]
    first = (n_obs - slabs) // 2
    steps = depart_ref.shape[0] // GROUPS
    chunk = GROUPS * LANES
    w = lax.axis_index("win")
    o = lax.axis_index("obs")

    barrier = pltpu.get_barrier_semaphore()
    for step in range(1, n_obs):
        pl.semaphore_signal(
            barrier, inc=1, device_id={"obs": lax.rem(o + step, n_obs)}, device_id_type=MESH
        )
    for step in range(1, n_win):
        pl.semaphore_signal(
            barrier, inc=1, device_id={"win": lax.rem(w + step, n_win)}, device_id_type=MESH
        )

    def loads(step):
        begin = pl.multiple_of(step * chunk, chunk)
        some = pl.ds(pl.multiple_of(step * GROUPS, GROUPS), GROUPS)
        return [
            pltpu.make_async_copy(
                rows_hbm.at[:, pl.ds(begin, chunk)],
                rows_ref.at[:, pl.ds(begin, chunk)],
                load_sem.at[0, step],
            ),
            pltpu.make_async_copy(depart_hbm.at[some], depart_ref.at[some], load_sem.at[1, step]),
            pltpu.make_async_copy(label_hbm.at[some], label_ref.at[some], load_sem.at[2, step]),
        ]

    def start_loads(step, carry):
        for load in loads(step):
            load.start()
        return carry

    lax.fori_loop(0, steps, start_loads, 0)

    def decay_copy(step, slot, target):
        return pltpu.make_async_remote_copy(
            src_ref=decays.at[slot],
            dst_ref=decays.at[slot],
            send_sem=decay_send.at[step],
            recv_sem=decay_recv.at[step],
            device_id={"win": target},
            device_id_type=MESH,
        )

    decays[w] = jnp.zeros((dim, width), jnp.float32)
    decays[w, :, 0:channels] = jnp.broadcast_to(decay_ref[...], (dim, channels))
    ridge_all[...] = jnp.ones_like(ridge_all)
    ridge_all[:, 0:channels] = ridge_ref[...].astype(jnp.float32)
    for slab in range(slabs):
        ridge_slab[slab] = ridge_all[:, slab * LANES : (slab + 1) * LANES]

    def tables_now(r):
        return [betas[r, slab] for slab in range(slabs)]

    def wide_row(ref, row):
        return jnp.broadcast_to(ref[pl.ds(row, 1), :], (dim, LANES))

    def accumulate(step, tables):
        fits, departs, labels = [], [], []
        columns_all = []
        for group in range(GROUPS):
            row = step * GROUPS + group
            begin = pl.multiple_of(row * LANES, LANES)
            columns = rows_ref[:, pl.ds(begin, LANES)]
            label = wide_row(label_ref, row)
            depart = wide_row(depart_ref, row)
            residual = depart
            if tables is not None:
                residual = depart - fit_group(columns, label, tables)
            weight = huber_edge / jnp.maximum(jnp.abs(residual), huber_edge)
            columns_all.append(columns)
            fits.append(columns * weight)
            departs.append(depart)
            labels.append(label)
        columns = jnp.concatenate(columns_all, axis=1)
        weighted = jnp.concatenate(fits, axis=1)
        depart = jnp.concatenate(departs, axis=1)
        label = jnp.concatenate(labels, axis=1)
        features = [weighted * columns]
        for shift in range(1, dim // 2 + 1):
            features.append(weighted * pltpu.roll(columns, shift, axis=0))
        features.append(weighted * depart)
        features = jnp.concatenate(features, axis=0)
        high = features.astype(jnp.bfloat16)
        low = (features - high.astype(jnp.float32)).astype(jnp.bfloat16)
        pair = jnp.concatenate([high, low], axis=0)
        upper = label >= half
        place = jnp.where(upper, label - half, label)
        place = place.astype(jnp.float32).astype(jnp.bfloat16)
        side = upper.astype(jnp.float32).astype(jnp.bfloat16)
        place = jnp.concatenate([place, place], axis=0)
        side = jnp.concatenate([side, side], axis=0)
        one, nought = jnp.bfloat16(1), jnp.bfloat16(0)
        is_upper = side > jnp.bfloat16(0.5)
        sides = [[], []]
        for part in range(0, 2 * packed, 2 * dim):
            tile = pair[part : part + 2 * dim]
            sides[0].append(jnp.where(is_upper, nought, tile))
            sides[1].append(jnp.where(is_upper, tile, nought))
        spread = jnp.concatenate(sides[0] + sides[1], axis=0)
        ids = lax.broadcasted_iota(jnp.int32, (half, LANES), 0)
        ids = ids.astype(jnp.float32).astype(jnp.bfloat16)
        hots = []
        for part in range(0, half, 2 * dim):
            id_tile = jnp.concatenate([ids[part : part + 2 * dim]] * GROUPS, axis=1)
            hots.append(jnp.where(id_tile == place, one, nought))
        hot = jnp.concatenate(hots, axis=0)
        acc[:, 0:half] += lax.dot_general(
            spread, hot, (((1,), (1,)), ((), ())), preferred_element_type=jnp.float32
        )

    def part_copy(r, slab, slot):
        return pltpu.make_async_remote_copy(
            src_ref=stats.at[slab],
            dst_ref=parts.at[r, slot],
            send_sem=part_send.at[r, slab],
            recv_sem=part_recv.at[r, slot],
            device_id={"obs": first + slab},
            device_id_type=MESH,
        )

    def total_copy(r, step, slot, target):
        return pltpu.make_async_remote_copy(
            src_ref=totals.at[r, slot],
            dst_ref=totals.at[r, slot],
            send_sem=total_send.at[r, step],
            recv_sem=total_recv.at[r, step],
            device_id={"win": target},
            device_id_type=MESH,
        )

    def beta_copy(r, step, slab, target):
        return pltpu.make_async_remote_copy(
            src_ref=betas.at[r, slab],
            dst_ref=betas.at[r, slab],
            send_sem=beta_send.at[r, step],
            recv_sem=beta_recv.at[r, slab],
            device_id={"obs": target},
            device_id_type=MESH,
        )

    def combine(r, opening=False):
        zeros = jnp.zeros((packed, width - acc.shape[1]), jnp.float32)
        sides = []
        for side in range(2):
            begin = side * 2 * packed
            both = acc[begin : begin + packed] + acc[begin + packed : begin + 2 * packed]
            sides.append(jnp.concatenate([both, zeros], axis=1))
        whole = sides[0] + pltpu.roll(sides[1], half, axis=1)
        for slab in range(slabs):
            stats[slab] = whole[:, slab * LANES : (slab + 1) * LANES]
        for slab in range(slabs):

            @pl.when(o != first + slab)
            def _():
                part_copy(r, slab, o).start()

        if opening:
            for step in range(1, n_win):
                decay_copy(step, lax.rem(w + n_win - step, n_win), w).wait_recv()
            for step in range(1, n_win):
                decay_copy(step, w, w).wait_send()

        for slab in range(slabs):

            @pl.when(o == first + slab)
            def _():
                parts[r, o] = stats[slab]
                for step in range(1, n_obs):
                    part_copy(r, 0, lax.rem(o + step, n_obs)).wait_recv()
                total = parts[r, 0]
                for source in range(1, n_obs):
                    total = total + parts[r, source]
                totals[r, w] = total
                for step in range(1, n_win):
                    total_copy(r, step, w, lax.rem(w + step, n_win)).start()
                for step in range(1, n_win):
                    total_copy(r, step, lax.rem(w + n_win - step, n_win), w).wait_recv()
                lanes = slice(slab * LANES, (slab + 1) * LANES)
                carried = totals[r, 0]
                for window in range(1, n_win):
                    decay = jnp.concatenate([decays[window, :, lanes]] * (packed // dim), axis=0)
                    further = decay * carried + totals[r, window]
                    carried = jnp.where(window <= w, further, carried)
                chained[...] = carried
                solve(r, slab)
                for step in range(1, n_obs):
                    beta_copy(r, step, slab, lax.rem(o + step, n_obs)).start()

        for slab in range(slabs):

            @pl.when(o != first + slab)
            def _():
                beta_copy(r, 1, slab, o).wait_recv()

        for slab in range(slabs):

            @pl.when(o != first + slab)
            def _():
                part_copy(r, slab, o).wait_send()

            @pl.when(o == first + slab)
            def _():
                for step in range(1, n_win):
                    total_copy(r, step, w, w).wait_send()
                for step in range(1, n_obs):
                    beta_copy(r, step, slab, o).wait_send()

    def solve(r, slab):
        def entry(place):
            return chained[place : place + 1, :]

        unit = {}
        scaled = {}
        inverse = []
        for column in range(dim):
            pivot = entry(entry_place(column, column, dim)) + ridge_slab[slab]
            for middle in range(column):
                pivot = pivot - unit[column, middle] * scaled[column, middle]
            inverse.append(1.0 / pivot)
            for row in range(column + 1, dim):
                value = entry(entry_place(row, column, dim))
                for middle in range(column):
                    value = value - unit[column, middle] * scaled[row, middle]
                scaled[row, column] = value
                unit[row, column] = value * inverse[column]
        forward = []
        moment = (dim // 2 + 1) * dim
        for row in range(dim):
            value = entry(moment + row)
            for middle in range(row):
                value = value - unit[row, middle] * forward[middle]
            forward.append(value)
        answer = [None] * dim
        for row in reversed(range(dim)):
            value = forward[row] * inverse[row]
            for middle in range(row + 1, dim):
                value = value - unit[middle, row] * answer[middle]
            answer[row] = value
            betas[r, slab, row : row + 1, :] = value

    acc[...] = jnp.zeros_like(acc)

    def opening_step(step, carry):
        for load in loads(step):
            load.wait()
        accumulate(step, None)
        return carry

    lax.fori_loop(0, steps, opening_step, 0)

    pl.semaphore_wait(barrier, n_obs + n_win - 2)
    for step in range(1, n_win):
        decay_copy(step, w, lax.rem(w + step, n_win)).start()
    combine(0, True)

    def one_round(r, carry):
        acc[...] = jnp.zeros_like(acc)
        tables = tables_now(r - 1)

        def one_step(step, inner):
            accumulate(step, tables)
            return inner

        lax.fori_loop(0, steps, one_step, 0)
        combine(r)
        return carry

    lax.fori_loop(1, ROUNDS, one_round, 0)

    tables = tables_now(ROUNDS - 1)
    coef_ref[...] = jnp.concatenate(tables, axis=1)[:, 0:channels]

    def correct(step, carry):
        for group in range(GROUPS):
            row = step * GROUPS + group
            begin = pl.multiple_of(row * LANES, LANES)
            columns = rows_ref[:, pl.ds(begin, LANES)]
            fitted = fit_group(columns, wide_row(label_ref, row), tables)
            corrected_ref[pl.ds(row, 1), :] = depart_ref[pl.ds(row, 1), :] - fitted
        return carry

    lax.fori_loop(0, steps, correct, 0)


def body(n_win, n_obs, predictors, departures, channel, decay_rate, ridge_counts):
    channels = decay_rate.shape[1]
    dim = predictors.shape[1]
    total_rows = predictors.shape[2]
    slabs = ceil_to(channels, LANES) // LANES
    width = slabs * LANES
    packed = (dim // 2 + 2) * dim
    half = ceil_to((channels + 1) // 2, 16)
    acc_width = ceil_to(half, LANES)
    steps = total_rows // (GROUPS * LANES)
    assert n_obs >= slabs and total_rows % (GROUPS * LANES) == 0
    assert half <= 256 and acc_width < width and 2 * half <= width
    vmem = pl.BlockSpec(memory_space=pltpu.VMEM)
    hbm = pl.BlockSpec(memory_space=pltpu.HBM)
    dma = pltpu.SemaphoreType.DMA
    lines = total_rows // LANES
    coeffs, corrected = pl.pallas_call(
        functools.partial(kernel, (dim, channels, n_win, n_obs, slabs, half)),
        out_shape=(
            jax.ShapeDtypeStruct((dim, channels), jnp.float32),
            jax.ShapeDtypeStruct((lines, LANES), jnp.float32),
        ),
        in_specs=[hbm] * 3 + [vmem] * 2,
        out_specs=(vmem, vmem),
        scratch_shapes=[
            pltpu.VMEM((dim, total_rows), jnp.float32),
            pltpu.VMEM((lines, LANES), jnp.float32),
            pltpu.VMEM((lines, LANES), jnp.int32),
            pltpu.VMEM((4 * packed, acc_width), jnp.float32),
            pltpu.VMEM((slabs, packed, LANES), jnp.float32),
            pltpu.VMEM((ROUNDS, slabs, dim, LANES), jnp.float32),
            pltpu.VMEM((1, width), jnp.float32),
            pltpu.VMEM((slabs, 1, LANES), jnp.float32),
            pltpu.VMEM((n_win, dim, width), jnp.float32),
            pltpu.VMEM((ROUNDS, n_obs, packed, LANES), jnp.float32),
            pltpu.VMEM((ROUNDS, n_win, packed, LANES), jnp.float32),
            pltpu.VMEM((packed, LANES), jnp.float32),
            dma((3, steps)),
            dma((n_win,)),
            dma((n_win,)),
            dma((ROUNDS, slabs)),
            dma((ROUNDS, n_obs)),
            dma((ROUNDS, n_win)),
            dma((ROUNDS, n_win)),
            dma((ROUNDS, n_obs)),
            dma((ROUNDS, slabs)),
        ],
        compiler_params=pltpu.CompilerParams(
            collective_id=0, has_side_effects=True, vmem_limit_bytes=48 * 1024 * 1024
        ),
    )(
        predictors.reshape(dim, total_rows),
        departures.reshape(lines, LANES),
        channel.reshape(lines, LANES),
        decay_rate,
        ridge_counts,
    )
    return (coeffs[None], corrected.reshape(1, total_rows))


def solution(mesh):
    placed = (
        P("win", None, "obs"),
        P("win", "obs"),
        P("win", "obs"),
        P("win", None),
        P("win", None),
    )
    return jax.shard_map(
        functools.partial(body, mesh.shape["win"], mesh.shape["obs"]),
        mesh=mesh,
        in_specs=placed,
        out_specs=(P("win", None, None), P("win", "obs")),
        check_vma=False,
    )
```
